32 devices in a mesh: groups: 2 (over x), blk: 8 (over z, y), heads: 2 (over core).
Axes of the slice: x: 2, y: 2, z: 4, core: 2. Of those that a mesh axis runs over, the one named last changes fastest.
Arguments:
- image_feats: bfloat16 [4096, 8192], P(('groups', 'blk')), parts along dimension 0, may hold values from -6 to 6
- slot_image: int32 [4096], P(('groups', 'blk')), parts along dimension 0, may hold values from -1 to 3, as said below
- key_weight: bfloat16 [8192, 512], P('blk', 'heads'), may hold values from -0.0625 to 0.0625
- value_weight: bfloat16 [8192, 512], P('blk', 'heads'), may hold values from -0.0625 to 0.0625
- key_gain: float32 [128], replicated, may hold values from 0.25 to 1.75
- queries: bfloat16 [512, 4096], P(('groups', 'blk'), 'heads'), parts along dimension 0, may hold values from -60 to 60
- text_image: int32 [512], P('groups'), parts along dimension 0, may hold values from 0 to 3
- text_hidden: bfloat16 [512, 8192], P(('groups', 'heads'), 'blk'), parts along dimension 0, may hold values from -4 to 4
- out_weight: bfloat16 [4096, 8192], P('heads', 'blk'), may hold values from -0.09375 to 0.09375
- attn_gate: float32 [1], replicated, may hold values from 0.4 to 1.2
Outputs:
- mixed: bfloat16 [512, 8192], P(('groups', 'heads'), 'blk'), parts along dimension 0
The draws below stay inside these ranges and needn't reach their ends.
There are 2 independent parts, one for each index of `groups`. The reference program is written for one: setup_inputs(seed, part) draws one part's arguments, and reference() takes and returns one part's arrays. A program takes and returns all parts, laid end to end along the dimension named above; an argument that names none is the same for every part. Nothing has to cross between parts.
Inputs may be any that keep to these rules, and one draw needn't show every extreme that they name: `slot_image`: slots come in tiles of 64; the live slots of a tile come first and carry one image id, -1 marks an empty slot; every image has live slots; the first 256 slots are all live.
All inputs are finite; a program needn't handle non-finite values.
Results may differ from the reference program's by a relative error of at most 0.008.
Values may be sent and summed in bfloat16 or wider, within the bound.
A program may use at most 128 MiB of HBM per device.

```python
import math
import jax
import jax.numpy as jnp
from jax import lax

D = 8192
DV = 8192
HQ = 32
KVH = 4
HD = 128
IMAGES = 4
TILE = 64
TOK_DEV = 256
IMG = 2048
TEXT = 256


def draw_slot_image(key, part):
    tile_count = IMG // TILE
    per_dev = TOK_DEV // TILE
    devices_count = tile_count // per_dev
    key_a, key_b, key_c, key_d = jax.random.split(jax.random.fold_in(key, 11), 4)
    fill_level = jax.random.randint(key_a, (devices_count,), 0, 8)
    tile_index = jnp.arange(tile_count)
    owner_dev = tile_index // per_dev
    first_tiles = tile_index < IMAGES
    live_tile = jax.random.randint(key_b, (tile_count,), 0, 10) < 3 + fill_level[owner_dev]
    live_tile = live_tile | (owner_dev == 0) | first_tiles
    image_id = jax.random.randint(key_c, (tile_count,), 0, IMAGES)
    image_id = jnp.where(first_tiles, tile_index % IMAGES, image_id)
    token_count = jax.random.randint(key_d, (tile_count,), TILE // 2, TILE + 1)
    token_count = jnp.where(owner_dev == 0, TILE, token_count)
    position = jnp.arange(TILE)
    slot_ids = jnp.where(live_tile[:, None] & (position[None, :] < token_count[:, None]), image_id[:, None], -1)
    return slot_ids.reshape(IMG).astype(jnp.int32)


def draw_queries(key, part):
    base = jax.random.normal(jax.random.fold_in(key, 23), (TEXT, HQ * HD), jnp.float32)
    drawn = jnp.clip(2.0 * base, -12.0, 12.0)
    return drawn.astype(jnp.bfloat16)


def plant(array, own_key, low, largest):
    dims = array.shape
    spot = [jax.random.randint(jax.random.fold_in(own_key, axis), (), 0, dims[axis]) for axis in range(len(dims))]
    array = array.at[tuple(spot)].set(low)
    longest = dims.index(max(dims))
    spot[longest] = (spot[longest] + 1) % dims[longest]
    return array.at[tuple(spot)].set(largest)


def block_scale(own_key, shape, pieces, low, top_value):
    def one(axis_at, parts):
        draws = jax.random.uniform(jax.random.fold_in(jax.random.fold_in(own_key, 6), axis_at), (parts,), jnp.float32, low / len(pieces), top_value / len(pieces))
        return jnp.repeat(jnp.exp(draws), shape[axis_at] // parts).reshape((-1,) + (1,) * (len(shape) - axis_at - 1))

    factor_of = one(*pieces[0])
    for cut in pieces[1:]:
        factor_of = factor_of * one(*cut)
    return factor_of


def bell_draw(rng, shape, deviation, limit, cuts=(), kind=jnp.bfloat16):
    values = jax.random.normal(rng, shape, jnp.float32) * deviation
    if len(cuts) > 0:
        values = block_scale(rng, shape, cuts, -0.22, 0.18) * values
    return jnp.clip(values, min=-limit, max=limit).astype(kind)


def setup_inputs(seed: int = 0, part: int = 0) -> dict:
    arg_keys = jax.random.split(jax.random.key(seed), 11)
    own_keys = jax.random.split(jax.random.fold_in(arg_keys[10], part), 11)
    image_feats = bell_draw(own_keys[0], (IMG, DV), 1.0, 6.0, ((0, 8),))
    slot_image = draw_slot_image(jax.random.fold_in(jax.random.fold_in(arg_keys[10], part), 71), part)
    key_weight = bell_draw(arg_keys[2], (DV, KVH * HD), DV ** -0.5, 0.0625, ((0, 8), (1, 2)))
    value_weight = bell_draw(arg_keys[3], (DV, KVH * HD), DV ** -0.5, 0.0625, ((0, 8), (1, 2)))
    key_gain = jnp.clip(1.0 + 0.15 * jax.random.normal(arg_keys[4], (HD,), jnp.float32), 0.25, 1.75)
    queries = draw_queries(jax.random.fold_in(jax.random.fold_in(arg_keys[10], part), 71), part)
    text_image = plant(jax.random.randint(own_keys[6], (TEXT,), 0, IMAGES), jax.random.fold_in(own_keys[6], 1), 0, IMAGES - 1).astype(jnp.int32)
    text_hidden = bell_draw(own_keys[7], (TEXT, D), 0.5, 4.0, ((0, 2), (1, 8)))
    out_weight = bell_draw(arg_keys[8], (HQ * HD, D), (HQ * HD) ** -0.5, 0.09375, ((0, 2), (1, 8)))
    attn_gate = jnp.clip(jax.random.uniform(arg_keys[9], (1,), jnp.float32, 0.4, 1.2), 0.4, 1.2)
    return dict(image_feats=image_feats, slot_image=slot_image, key_weight=key_weight, value_weight=value_weight, key_gain=key_gain, queries=queries, text_image=text_image, text_hidden=text_hidden, out_weight=out_weight, attn_gate=attn_gate)


def reference(image_feats, slot_image, key_weight, value_weight, key_gain, queries, text_image, text_hidden, out_weight, attn_gate):
    keys_raw = jnp.dot(image_feats, key_weight, preferred_element_type=jnp.float32).reshape(IMG, KVH, HD)
    norm_scale = lax.rsqrt(lax.optimization_barrier(jnp.mean(keys_raw * keys_raw, axis=-1, keepdims=True)) + 1e-05)
    keys = (keys_raw * norm_scale * key_gain).astype(jnp.bfloat16)
    values = jnp.dot(image_feats, value_weight, preferred_element_type=jnp.float32).astype(jnp.bfloat16).reshape(IMG, KVH, HD)
    visible = (slot_image[None, :] >= 0) & (slot_image[None, :] <= text_image[:, None])
    score_scale = 1.0 / math.sqrt(HD)
    per_kv = HQ // KVH

    def one_head(head):
        group_id = head // per_kv
        query_head = lax.dynamic_slice_in_dim(queries, head * HD, HD, 1)
        key_head = lax.dynamic_index_in_dim(keys, group_id, 1, keepdims=False)
        value_head = lax.dynamic_index_in_dim(values, group_id, 1, keepdims=False)
        scores = jnp.dot(query_head, key_head.T, preferred_element_type=jnp.float32) * score_scale
        row_top = lax.optimization_barrier(jnp.max(jnp.where(visible, scores, -1e+30), axis=1, keepdims=True))
        expo = jnp.where(visible, jnp.exp(scores - row_top), 0.0)
        numerator = jnp.dot(expo.astype(jnp.bfloat16), value_head, preferred_element_type=jnp.float32)
        return (numerator / lax.optimization_barrier(jnp.sum(expo, axis=1, keepdims=True))).astype(jnp.bfloat16)
    heads_out = lax.map(one_head, jnp.arange(HQ).astype(jnp.int32))
    attn = jnp.transpose(heads_out, (1, 0, 2)).reshape(TEXT, HQ * HD)
    proj = jnp.dot(attn, out_weight, preferred_element_type=jnp.float32)
    return (text_hidden.astype(jnp.float32) + jnp.tanh(attn_gate[0]) * proj).astype(jnp.bfloat16)
```

```python
import functools
import math

import jax
import jax.numpy as jnp
from jax import lax
from jax.experimental import pallas as pl
from jax.experimental.pallas import tpu as pltpu
from jax.sharding import PartitionSpec as P

HD = 128
F32 = jnp.float32
BF16 = jnp.bfloat16
MESH = pl.DeviceIdType.MESH


def kernel(
    nb,
    chunks,
    feats,
    kw,
    vw,
    gain,
    codes,
    queries,
    rowimg,
    hidden,
    wout,
    gate,
    out,
    wbuf,
    fown,
    fnbr,
    acc_own,
    acc_nbr,
    psend,
    precv,
    pbuf,
    gbuf,
    qbuf,
    qall,
    sbuf,
    mbuf,
    lbuf,
    obuf,
    agbuf,
    wov,
    part,
    xsend,
    xrecv,
    lsem,
    fsem,
    wz_send,
    wx_send,
    w_recv,
    f_send,
    ff_send,
    f_recv,
    q_sem,
    p_send,
    p_recv,
    k_send,
    kf_send,
    k_recv,
    a_send,
    af_send,
    a_recv,
    x_sem,
):
    Y = 2
    Z = nb // Y
    ZH = Z // 2
    half = nb // 2
    g = lax.axis_index("groups")
    b = lax.axis_index("blk")
    c = lax.axis_index("heads")
    z = b // Y
    y = b % Y
    h = z // ZH
    r = (z % ZH) * Y + y
    gp = g % 2
    gx = g + 1 - 2 * gp
    tok, dv = feats.shape
    S, kc = kw.shape
    rows, qc = queries.shape
    gc = qc // 2
    qpk = gc // HD
    R2 = 2 * rows
    CR = S // chunks
    ybro = {"blk": z * Y + 1 - y}
    xbro = {"groups": gx}
    cbro = {"heads": 1 - c}
    qbro = (1 - h) * half + r
    pending = []

    def remote(src, dst, ssem, rsem, dev):
        return pltpu.make_async_remote_copy(
            src_ref=src, dst_ref=dst, send_sem=ssem, recv_sem=rsem, device_id=dev, device_id_type=MESH
        )

    def send(cond, *args):
        copy = remote(*args)
        if cond is None:
            copy.start()
        else:
            pl.when(cond)(lambda: copy.start())
        pending.append((cond, copy))

    def arrived(ref, sem):
        pltpu.make_async_copy(ref, ref, sem).wait()

    own_k = pltpu.make_async_copy(kw, wbuf.at[0, z], lsem.at[0])
    own_v = pltpu.make_async_copy(vw, wbuf.at[1, z], lsem.at[1])
    own_k.start()
    own_v.start()

    barrier = pltpu.get_barrier_semaphore()
    for zd in range(Z):

        @pl.when(zd != z)
        def _():
            pl.semaphore_signal(barrier, inc=1, device_id={"blk": zd * Y + y}, device_id_type=MESH)

    for dev in (ybro, xbro, cbro):
        pl.semaphore_signal(barrier, inc=1, device_id=dev, device_id_type=MESH)
    own_k.wait()
    own_v.wait()
    pl.semaphore_wait(barrier, Z + 2)

    def wslot(kv, zi, ci):
        return wbuf.at[kv, zi, pl.ds(ci * CR, CR), :]

    for ci in range(chunks):
        for dirn, ok in ((1, z + 1 < Z), (-1, z >= 1)):
            slot = wslot(gp, z, ci)
            send(
                ok,
                slot,
                slot,
                wz_send.at[z, ci, (1 - dirn) // 2],
                w_recv.at[gp, z, ci],
                {"blk": b + dirn * Y},
            )

    FB = Z // 2
    for i in range(FB):
        zi = 2 * i + c
        send(
            None,
            feats.at[:, pl.ds(pl.multiple_of((zi * Y + 1 - y) * S, S), S)],
            fnbr.at[zi],
            f_send.at[i],
            f_recv.at[zi],
            ybro,
        )
    send(
        None,
        queries.at[:, pl.ds(pl.multiple_of((1 - h) * gc, gc), gc)],
        qbuf.at[h],
        q_sem.at[0],
        q_sem.at[1],
        {"blk": qbro},
    )
    floc = []
    for zi in range(Z):
        cp = pltpu.make_async_copy(
            feats.at[:, pl.ds(pl.multiple_of((zi * Y + y) * S, S), S)], fown.at[zi], fsem.at[zi]
        )
        cp.start()
        floc.append(cp)
    qloc = pltpu.make_async_copy(
        queries.at[:, pl.ds(pl.multiple_of(h * gc, gc), gc)], qbuf.at[h], lsem.at[2]
    )
    qloc.start()
    woloc = pltpu.make_async_copy(wout, wov, lsem.at[3])
    woloc.start()

    acc_own[...] = jnp.zeros_like(acc_own)
    acc_nbr[...] = jnp.zeros_like(acc_nbr)

    def mm(acc, feat, zi):
        for kv in range(2):
            acc[:, kv * kc : (kv + 1) * kc] += jnp.dot(
                feat[zi], wbuf[kv, zi], preferred_element_type=F32
            )

    for cp in floc:
        cp.wait()

    def sides(s):
        return ((z - s, z - s >= 0, -1), (z + s, z + s < Z, 1))

    for s in range(1, Z):
        for ci in range(chunks):
            for zi, ok, side in sides(s):
                slot = wslot(gp, zi, ci)
                pl.when(ok)(lambda: arrived(slot, w_recv.at[gp, zi, ci]))
                onward = b - side * Y
                more = ok & ((z + 1 < Z) if side < 0 else (z >= 1))
                send(more, slot, slot, wz_send.at[zi, ci, 0], w_recv.at[gp, zi, ci], {"blk": onward})
                send(ok, slot, slot, wx_send.at[zi, ci], w_recv.at[gp, zi, ci], xbro)
        if s - 1 < FB:
            zi = 2 * (s - 1) + c
            arrived(fnbr.at[zi], f_recv.at[zi])
            send(None, fnbr.at[zi], fnbr.at[zi], ff_send.at[s - 1], f_recv.at[zi], cbro)
        if s == 1:
            mm(acc_own, fown, z)
        else:
            for zi, ok, _ in sides(s - 1):

                @pl.when(ok)
                def _():
                    for ci in range(chunks):
                        arrived(wslot(1 - gp, zi, ci), w_recv.at[1 - gp, zi, ci])
                    mm(acc_own, fown, zi)

    for i in range(FB):
        zi = 2 * i + 1 - c
        arrived(fnbr.at[zi], f_recv.at[zi])
    for zi, ok, _ in sides(Z - 1):

        @pl.when(ok)
        def _():
            for ci in range(chunks):
                arrived(wslot(1 - gp, zi, ci), w_recv.at[1 - gp, zi, ci])

    @pl.loop(0, Z)
    def _(zi):
        mm(acc_nbr, fnbr, zi)

    psend[...] = acc_nbr[...].astype(BF16)
    send(None, psend, precv, p_send, p_recv, ybro)
    for zi, ok, _ in sides(Z - 1):
        pl.when(ok)(lambda: mm(acc_own, fown, zi))
    arrived(precv, p_recv)

    total = acc_own[...] + precv[...].astype(F32)
    for hh in range(2):
        kr = total[:, hh * HD : (hh + 1) * HD]
        scale = lax.rsqrt(jnp.mean(kr * kr, axis=-1, keepdims=True) + 1e-05)
        pbuf[hh, 0:tok, :] = (kr * scale * gain[...]).astype(BF16)
        pbuf[hh, tok : 2 * tok, :] = total[:, kc + hh * HD : kc + (hh + 1) * HD].astype(BF16)
        pbuf[hh, 2 * tok :, :] = codes[...]
    gbuf[b] = pbuf[h]
    for zd in range(Z):
        send(
            zd != z,
            pbuf.at[zd // ZH],
            gbuf.at[b],
            k_send.at[zd],
            k_recv.at[b],
            {"blk": zd * Y + y},
        )

    def collect(slot_of, fsend, recv):
        for s in range(Z):
            for zi, ok, _ in sides(s)[: 1 if s == 0 else 2]:
                bi = zi * Y + y
                if s > 0:
                    pl.when(ok)(lambda: arrived(slot_of(bi), recv.at[bi]))
                send(
                    None if s == 0 else ok, slot_of(bi), slot_of(bi), fsend.at[zi], recv.at[bi], ybro
                )
        for zi in range(Z):
            bi = zi * Y + 1 - y
            arrived(slot_of(bi), recv.at[bi])

    collect(lambda bi: gbuf.at[bi], kf_send, k_recv)

    qloc.wait()
    arrived(qbuf.at[1 - h], q_sem.at[1])
    for j in range(qpk):
        for so in range(2):
            at = j * R2 + so * rows
            qall[at : at + rows, :] = qbuf[so, :, j * HD : (j + 1) * HD]
    mbuf[...] = jnp.full_like(mbuf, -1e30)
    lbuf[...] = jnp.zeros_like(lbuf)
    obuf[...] = jnp.zeros_like(obuf)
    score_scale = 1.0 / math.sqrt(HD)

    @pl.loop(0, nb)
    def _(bi):
        code = gbuf[bi, 2 * tok :, :].astype(F32)
        img = jnp.concatenate([rowimg[...]] * qpk, axis=0)
        for t in range(tok // HD):
            s = (
                lax.dot_general(
                    qall[...],
                    gbuf[bi, t * HD : (t + 1) * HD, :],
                    (((1,), (1,)), ((), ())),
                    preferred_element_type=F32,
                )
                * score_scale
            )
            crow = code[t : t + 1, :]
            s = jnp.where((crow >= 0.0) & (crow <= img), s, -1e30)
            sbuf[bi, t] = s
            mbuf[...] = jnp.maximum(mbuf[...], s)

    mbuf[...] = jnp.broadcast_to(jnp.max(mbuf[...], axis=1, keepdims=True), mbuf.shape)

    @pl.loop(0, nb)
    def _(bi):
        top = mbuf[...]
        ps = [jnp.exp(sbuf[bi, t] - top) for t in range(tok // HD)]
        for p in ps:
            lbuf[...] += p
        obuf[...] += jnp.dot(
            jnp.concatenate([p.astype(BF16) for p in ps], axis=1),
            gbuf[bi, tok : 2 * tok, :],
            preferred_element_type=F32,
        )

    attn = (obuf[...] / jnp.sum(lbuf[...], axis=1, keepdims=True)).astype(BF16)
    for j in range(qpk):
        for so in range(2):
            at = j * R2 + so * rows
            agbuf[h, so, r, :, j * HD : (j + 1) * HD] = attn[at : at + rows, :]

    def aslot(bi):
        zz = bi // Y
        return agbuf.at[zz // ZH, :, (zz % ZH) * Y + bi % Y]

    for zd in range(Z):
        send(zd != z, aslot(b), aslot(b), a_send.at[zd], a_recv.at[b], {"blk": zd * Y + y})
    collect(aslot, af_send, a_recv)

    woloc.wait()
    hrows = half * rows

    def proj(so):
        a0 = agbuf[0, so].reshape(hrows, gc)
        a1 = agbuf[1, so].reshape(hrows, gc)
        return jnp.dot(a0, wov[0:gc, :], preferred_element_type=F32) + jnp.dot(
            a1, wov[gc:, :], preferred_element_type=F32
        )

    xsend[...] = proj(1 - c).astype(BF16)
    send(None, xsend, xrecv, x_sem.at[0], x_sem.at[1], cbro)
    part[...] = proj(c)
    arrived(xrecv, x_sem.at[1])
    out[...] = (
        hidden[...].astype(F32) + jnp.tanh(gate[0:1, 0:1]) * (part[...] + xrecv[...].astype(F32))
    ).astype(BF16)

    for cond, copy in pending:
        if cond is None:
            copy.wait_send()
        else:
            pl.when(cond)(lambda: copy.wait_send())


def body(
    nb,
    image_feats,
    slot_image,
    key_weight,
    value_weight,
    key_gain,
    queries,
    text_image,
    text_hidden,
    out_weight,
    attn_gate,
):
    Z = nb // 2
    ZH = Z // 2
    half = nb // 2
    tok, dv = image_feats.shape
    S, kc = key_weight.shape
    rows, qc = queries.shape
    gc = qc // 2
    qpk = gc // HD
    M = qpk * 2 * rows
    trows, ocols = text_hidden.shape
    chunks = 4
    b = lax.axis_index("blk")
    r = b % half
    img = text_image.astype(F32).reshape(2, half, rows)
    img = lax.dynamic_index_in_dim(img, r, 1, keepdims=False).reshape(2 * rows, 1)
    rowimg = jnp.broadcast_to(img, (2 * rows, HD))
    codes = jnp.pad(
        slot_image.astype(BF16).reshape(tok // HD, HD),
        ((0, 16 - tok // HD), (0, 0)),
        constant_values=-1,
    )
    gate = jnp.broadcast_to(attn_gate.reshape(1, 1), (1, HD))
    pay = 2 * tok + 16
    any_spec = pl.BlockSpec(memory_space=pl.ANY)
    vspec = pl.BlockSpec(memory_space=pltpu.VMEM)
    dma = pltpu.SemaphoreType.DMA
    V = pltpu.VMEM
    return pl.pallas_call(
        functools.partial(kernel, nb, chunks),
        out_shape=jax.ShapeDtypeStruct((trows, ocols), BF16),
        in_specs=[
            any_spec,
            any_spec,
            any_spec,
            vspec,
            vspec,
            any_spec,
            vspec,
            vspec,
            any_spec,
            vspec,
        ],
        out_specs=vspec,
        scratch_shapes=[
            V((2, Z, S, kc), BF16),
            V((Z, tok, S), BF16),
            V((Z, tok, S), BF16),
            V((tok, 2 * kc), F32),
            V((tok, 2 * kc), F32),
            V((tok, 2 * kc), BF16),
            V((tok, 2 * kc), BF16),
            V((2, pay, HD), BF16),
            V((nb, pay, HD), BF16),
            V((2, rows, gc), BF16),
            V((M, HD), BF16),
            V((nb, tok // HD, M, HD), F32),
            V((M, HD), F32),
            V((M, HD), F32),
            V((M, HD), F32),
            V((2, 2, half, rows, gc), BF16),
            V(out_weight.shape, BF16),
            V((trows, ocols), F32),
            V((trows, ocols), BF16),
            V((trows, ocols), BF16),
            dma((4,)),
            dma((Z,)),
            dma((Z, chunks, 2)),
            dma((Z, chunks)),
            dma((2, Z, chunks)),
            dma((Z // 2,)),
            dma((Z // 2,)),
            dma((Z,)),
            dma((2,)),
            dma,
            dma,
            dma((Z,)),
            dma((Z,)),
            dma((nb,)),
            dma((Z,)),
            dma((Z,)),
            dma((nb,)),
            dma((2,)),
        ],
        compiler_params=pltpu.CompilerParams(
            collective_id=0, has_side_effects=True, vmem_limit_bytes=60 * 1024 * 1024
        ),
    )(
        image_feats,
        key_weight,
        value_weight,
        key_gain.reshape(1, HD),
        codes,
        queries,
        rowimg,
        text_hidden,
        out_weight,
        gate,
    )


def solution(mesh):
    placed = (
        P(("groups", "blk"), None),
        P(("groups", "blk")),
        P("blk", "heads"),
        P("blk", "heads"),
        P(),
        P(("groups", "blk"), "heads"),
        P("groups"),
        P(("groups", "heads"), "blk"),
        P("heads", "blk"),
        P(),
    )
    return jax.shard_map(
        functools.partial(body, mesh.shape["blk"]),
        mesh=mesh,
        in_specs=placed,
        out_specs=P(("groups", "heads"), "blk"),
        check_vma=False,
    )
```

```python
import functools
import math

import jax
import jax.numpy as jnp
from jax import lax
from jax.experimental import pallas as pl
from jax.experimental.pallas import tpu as pltpu
from jax.sharding import PartitionSpec as P

HD = 128
F32 = jnp.float32
BF16 = jnp.bfloat16
MESH = pl.DeviceIdType.MESH


def kernel(
    nb,
    chunks,
    feats,
    kw,
    vw,
    gain,
    slots,
    queries,
    text,
    hidden,
    wout,
    gate,
    out,
    wbuf,
    fown,
    fnbr,
    acc_own,
    acc_nbr,
    psend,
    precv,
    pbuf,
    gbuf,
    qbuf,
    qall,
    sbuf,
    mbuf,
    img,
    agbuf,
    wov,
    part,
    xsend,
    xrecv,
    lsem,
    fsem,
    wz_send,
    wx_send,
    w_recv,
    f_send,
    ff_send,
    f_recv,
    q_sem,
    p_send,
    p_recv,
    k_send,
    kf_send,
    k_recv,
    az_send,
    af_send,
    a_recv,
    x_sem,
):
    Y = 2
    Z = nb // Y
    ZH = Z // 2
    half = nb // 2
    g = lax.axis_index("groups")
    b = lax.axis_index("blk")
    c = lax.axis_index("heads")
    z = b // Y
    y = b % Y
    h = z // ZH
    r = (z % ZH) * Y + y
    gp = g % 2
    gx = g + 1 - 2 * gp
    tok, dv = feats.shape
    S, kc = kw.shape
    rows, qc = queries.shape
    gc = qc // 2
    qpk = gc // HD
    R2 = 2 * rows
    CR = S // chunks
    ybro = {"blk": z * Y + 1 - y}
    xbro = {"groups": gx}
    cbro = {"heads": 1 - c}
    qbro = (1 - h) * half + r
    pending = []

    def remote(src, dst, ssem, rsem, dev):
        return pltpu.make_async_remote_copy(
            src_ref=src, dst_ref=dst, send_sem=ssem, recv_sem=rsem, device_id=dev, device_id_type=MESH
        )

    def send(cond, *args):
        copy = remote(*args)
        if cond is None:
            copy.start()
        else:
            pl.when(cond)(lambda: copy.start())
        pending.append((cond, copy))

    def arrived(ref, sem):
        pltpu.make_async_copy(ref, ref, sem).wait()

    own_k = pltpu.make_async_copy(kw, wbuf.at[0, z], lsem.at[0])
    own_v = pltpu.make_async_copy(vw, wbuf.at[1, z], lsem.at[1])
    own_k.start()
    own_v.start()

    barrier = pltpu.get_barrier_semaphore()
    for zd in range(Z):

        @pl.when(zd != z)
        def _():
            pl.semaphore_signal(barrier, inc=1, device_id={"blk": zd * Y + y}, device_id_type=MESH)

    for dev in (ybro, xbro, cbro):
        pl.semaphore_signal(barrier, inc=1, device_id=dev, device_id_type=MESH)
    own_k.wait()
    own_v.wait()
    pl.semaphore_wait(barrier, Z + 2)

    def wslot(kv, zi, ci):
        return wbuf.at[kv, zi, pl.ds(ci * CR, CR), :]

    for ci in range(chunks):
        for dirn, ok in ((1, z + 1 < Z), (-1, z >= 1)):
            slot = wslot(gp, z, ci)
            send(
                ok,
                slot,
                slot,
                wz_send.at[z, ci, (1 - dirn) // 2],
                w_recv.at[gp, z, ci],
                {"blk": b + dirn * Y},
            )

    FB = Z // 2
    for i in range(FB):
        zi = 2 * i + c
        send(
            None,
            feats.at[:, pl.ds(pl.multiple_of((zi * Y + 1 - y) * S, S), S)],
            fnbr.at[zi],
            f_send.at[i],
            f_recv.at[zi],
            ybro,
        )
    send(
        None,
        queries.at[:, pl.ds(pl.multiple_of((1 - h) * gc, gc), gc)],
        qbuf.at[h],
        q_sem.at[0],
        q_sem.at[1],
        {"blk": qbro},
    )
    floc = []
    for zi in range(Z):
        cp = pltpu.make_async_copy(
            feats.at[:, pl.ds(pl.multiple_of((zi * Y + y) * S, S), S)], fown.at[zi], fsem.at[zi]
        )
        cp.start()
        floc.append(cp)
    qloc = pltpu.make_async_copy(
        queries.at[:, pl.ds(pl.multiple_of(h * gc, gc), gc)], qbuf.at[h], lsem.at[2]
    )
    qloc.start()
    woloc = pltpu.make_async_copy(wout, wov, lsem.at[3])
    woloc.start()

    acc_own[...] = jnp.zeros_like(acc_own)
    acc_nbr[...] = jnp.zeros_like(acc_nbr)

    def mm(acc, feat, zi):
        for kv in range(2):
            acc[:, kv * kc : (kv + 1) * kc] += jnp.dot(
                feat[zi], wbuf[kv, zi], preferred_element_type=F32
            )

    for cp in floc:
        cp.wait()

    def sides(s):
        return ((z - s, z - s >= 0, -1), (z + s, z + s < Z, 1))

    for s in range(1, Z):
        for ci in range(chunks):
            for zi, ok, side in sides(s):
                slot = wslot(gp, zi, ci)
                pl.when(ok)(lambda: arrived(slot, w_recv.at[gp, zi, ci]))
                onward = b - side * Y
                more = ok & ((z + 1 < Z) if side < 0 else (z >= 1))
                send(more, slot, slot, wz_send.at[zi, ci, 0], w_recv.at[gp, zi, ci], {"blk": onward})
                send(ok, slot, slot, wx_send.at[zi, ci], w_recv.at[gp, zi, ci], xbro)
        if s - 1 < FB:
            zi = 2 * (s - 1) + c
            arrived(fnbr.at[zi], f_recv.at[zi])
            send(None, fnbr.at[zi], fnbr.at[zi], ff_send.at[s - 1], f_recv.at[zi], cbro)
        if s == 1:
            mm(acc_own, fown, z)
        else:
            for zi, ok, _ in sides(s - 1):

                @pl.when(ok)
                def _():
                    for ci in range(chunks):
                        arrived(wslot(1 - gp, zi, ci), w_recv.at[1 - gp, zi, ci])
                    mm(acc_own, fown, zi)

    for i in range(FB):
        zi = 2 * i + 1 - c
        arrived(fnbr.at[zi], f_recv.at[zi])
    for zi, ok, _ in sides(Z - 1):

        @pl.when(ok)
        def _():
            for ci in range(chunks):
                arrived(wslot(1 - gp, zi, ci), w_recv.at[1 - gp, zi, ci])

    TC = tok // HD
    for t in range(TC):
        lo, hi = t * HD, (t + 1) * HD

        @pl.loop(0, Z)
        def _(zi):
            for kv in range(2):
                acc_nbr[lo:hi, kv * kc : (kv + 1) * kc] += jnp.dot(
                    fnbr[zi, lo:hi, :], wbuf[kv, zi], preferred_element_type=F32
                )

        psend[t] = acc_nbr[lo:hi, :].astype(BF16)
        send(None, psend.at[t], precv.at[t], p_send.at[t], p_recv.at[t], ybro)
    for zi, ok, _ in sides(Z - 1):
        pl.when(ok)(lambda: mm(acc_own, fown, zi))

    for t in range(TC):
        arrived(precv.at[t], p_recv.at[t])
        total = acc_own[t * HD : (t + 1) * HD, :] + precv[t].astype(F32)
        code = jnp.broadcast_to(slots[t : t + 1, :].astype(F32), (16, HD)).astype(BF16)
        for hh in range(2):
            kr = total[:, hh * HD : (hh + 1) * HD]
            scale = lax.rsqrt(jnp.mean(kr * kr, axis=-1, keepdims=True) + 1e-05)
            pbuf[hh, t, 0:HD, :] = (kr * scale * gain[...]).astype(BF16)
            pbuf[hh, t, HD : 2 * HD, :] = total[:, kc + hh * HD : kc + (hh + 1) * HD].astype(BF16)
            pbuf[hh, t, 2 * HD :, :] = code
        gbuf[b, t] = pbuf[h, t]
        for zd in range(Z):
            send(
                zd != z,
                pbuf.at[zd // ZH, t],
                gbuf.at[b, t],
                k_send.at[zd, t],
                k_recv.at[b, t],
                {"blk": zd * Y + y},
            )
        send(None, gbuf.at[b, t], gbuf.at[b, t], kf_send.at[z, t], k_recv.at[b, t], ybro)

    qloc.wait()
    arrived(qbuf.at[1 - h], q_sem.at[1])
    for j in range(qpk):
        for so in range(2):
            at = j * R2 + so * rows
            qall[at : at + rows, :] = qbuf[so, :, j * HD : (j + 1) * HD]
    count = text.shape[1]
    lane = lax.broadcasted_iota(jnp.int32, (R2, count), 1)
    sub = lax.broadcasted_iota(jnp.int32, (R2, count), 0)
    want = jnp.where(sub < rows, sub, sub + (half - 1) * rows) + r * rows
    picked = jnp.where(lane == want, text[...].astype(F32), 0.0)
    rowcol = jnp.broadcast_to(jnp.sum(picked, axis=1, keepdims=True), (R2, HD))
    for j in range(qpk):
        img[j * R2 : (j + 1) * R2, :] = rowcol
    mbuf[...] = jnp.full_like(mbuf, -1e30)
    score_scale = 1.0 / math.sqrt(HD)

    def score(bi):
        top = mbuf[...]
        for t in range(TC):
            s = (
                lax.dot_general(
                    qall[...],
                    gbuf[bi, t, 0:HD, :],
                    (((1,), (1,)), ((), ())),
                    preferred_element_type=F32,
                )
                * score_scale
            )
            crow = gbuf[bi, t, 2 * HD :, :].astype(F32)[0:1, :]
            s = jnp.where((crow >= 0.0) & (crow <= img[...]), s, -1e30)
            sbuf[bi, t] = s
            top = jnp.maximum(top, s)
        mbuf[...] = top

    for s in range(1, Z):
        for t in range(TC):
            for zi, ok, _ in sides(s):
                slot = gbuf.at[zi * Y + y, t]
                sem = k_recv.at[zi * Y + y, t]
                pl.when(ok)(lambda: arrived(slot, sem))
                send(ok, slot, slot, kf_send.at[zi, t], sem, ybro)

    @pl.loop(0, Z)
    def _(zi):
        score(zi * Y + y)

    @pl.loop(0, Z)
    def _(zi):
        for t in range(TC):
            arrived(gbuf.at[zi * Y + 1 - y, t], k_recv.at[zi * Y + 1 - y, t])
        score(zi * Y + 1 - y)

    NC = agbuf.shape[1]
    HC = qpk // NC
    MC = HC * R2

    def aslot(bi, jc):
        zz = bi // Y
        return agbuf.at[zz // ZH, jc, :, (zz % ZH) * Y + bi % Y]

    for jc in range(NC):
        r0, r1 = jc * MC, (jc + 1) * MC
        top = jnp.max(mbuf[r0:r1, :], axis=1, keepdims=True)

        def step(bi, carry):
            tot, acc = carry
            ps = [jnp.exp(sbuf[bi, t, r0:r1, :] - top) for t in range(TC)]
            for p in ps:
                tot = tot + p
            acc = acc + jnp.dot(
                jnp.concatenate([p.astype(BF16) for p in ps], axis=1),
                jnp.concatenate([gbuf[bi, t, HD : 2 * HD, :] for t in range(TC)], axis=0),
                preferred_element_type=F32,
            )
            return tot, acc

        zero = jnp.zeros((MC, HD), F32)
        tot, acc = lax.fori_loop(0, nb, step, (zero, zero))
        attn = (acc / jnp.sum(tot, axis=1, keepdims=True)).astype(BF16)
        for jj in range(HC):
            for so in range(2):
                at = jj * R2 + so * rows
                agbuf[h, jc, so, r, :, jj * HD : (jj + 1) * HD] = attn[at : at + rows, :]
        slot = aslot(b, jc)
        sem = a_recv.at[b, jc]
        send(z + 1 < Z, slot, slot, az_send.at[z, jc, 0], sem, {"blk": b + Y})
        send(z >= 1, slot, slot, az_send.at[z, jc, 1], sem, {"blk": b - Y})
        send(None, slot, slot, af_send.at[z, jc], sem, ybro)

    for s in range(1, Z):
        for jc in range(NC):
            for zi, ok, side in sides(s):
                bi = zi * Y + y
                slot = aslot(bi, jc)
                sem = a_recv.at[bi, jc]
                pl.when(ok)(lambda: arrived(slot, sem))
                more = ok & ((z + 1 < Z) if side < 0 else (z >= 1))
                send(more, slot, slot, az_send.at[zi, jc, 0], sem, {"blk": b - side * Y})
                send(ok, slot, slot, af_send.at[zi, jc], sem, ybro)
    for zi in range(Z):
        for jc in range(NC):
            bi = zi * Y + 1 - y
            arrived(aslot(bi, jc), a_recv.at[bi, jc])

    woloc.wait()
    hrows = half * rows
    ocols = out.shape[1]

    def proj(so):
        a = [agbuf[hh, jc, so].reshape(hrows, HC * HD) for hh in range(2) for jc in range(NC)]
        return jnp.dot(jnp.concatenate(a, axis=1), wov[...], preferred_element_type=F32)

    xsend[...] = proj(1 - c).astype(BF16)
    send(None, xsend, xrecv, x_sem.at[0], x_sem.at[1], cbro)
    part[...] = proj(c)
    arrived(xrecv, x_sem.at[1])
    out[...] = (
        hidden[...].astype(F32) + jnp.tanh(jnp.full((1, ocols), gate[0], F32)) * (part[...] + xrecv[...].astype(F32))
    ).astype(BF16)

    for cond, copy in pending:
        if cond is None:
            copy.wait_send()
        else:
            pl.when(cond)(lambda: copy.wait_send())


def body(
    nb,
    image_feats,
    slot_image,
    key_weight,
    value_weight,
    key_gain,
    queries,
    text_image,
    text_hidden,
    out_weight,
    attn_gate,
):
    Z = nb // 2
    ZH = Z // 2
    half = nb // 2
    tok, dv = image_feats.shape
    S, kc = key_weight.shape
    rows, qc = queries.shape
    gc = qc // 2
    qpk = gc // HD
    M = qpk * 2 * rows
    trows, ocols = text_hidden.shape
    chunks = 8 if S % 128 == 0 else 4
    TC = tok // HD
    NC = max(1, qpk // 2)
    any_spec = pl.BlockSpec(memory_space=pl.ANY)
    vspec = pl.BlockSpec(memory_space=pltpu.VMEM)
    dma = pltpu.SemaphoreType.DMA
    V = pltpu.VMEM
    return pl.pallas_call(
        functools.partial(kernel, nb, chunks),
        out_shape=jax.ShapeDtypeStruct((trows, ocols), BF16),
        in_specs=[
            any_spec,
            any_spec,
            any_spec,
            vspec,
            vspec,
            any_spec,
            vspec,
            vspec,
            any_spec,
            pl.BlockSpec(memory_space=pltpu.SMEM),
        ],
        out_specs=vspec,
        scratch_shapes=[
            V((2, Z, S, kc), BF16),
            V((Z, tok, S), BF16),
            V((Z, tok, S), BF16),
            V((tok, 2 * kc), F32),
            V((tok, 2 * kc), F32),
            V((TC, HD, 2 * kc), BF16),
            V((TC, HD, 2 * kc), BF16),
            V((2, TC, 2 * HD + 16, HD), BF16),
            V((nb, TC, 2 * HD + 16, HD), BF16),
            V((2, rows, gc), BF16),
            V((M, HD), BF16),
            V((nb, tok // HD, M, HD), F32),
            V((M, HD), F32),
            V((M, HD), F32),
            V((2, NC, 2, half, rows, gc // NC), BF16),
            V(out_weight.shape, BF16),
            V((trows, ocols), F32),
            V((trows, ocols), BF16),
            V((trows, ocols), BF16),
            dma((4,)),
            dma((Z,)),
            dma((Z, chunks, 2)),
            dma((Z, chunks)),
            dma((2, Z, chunks)),
            dma((Z // 2,)),
            dma((Z // 2,)),
            dma((Z,)),
            dma((2,)),
            dma((TC,)),
            dma((TC,)),
            dma((Z, TC)),
            dma((Z, TC)),
            dma((nb, TC)),
            dma((Z, NC, 2)),
            dma((Z, NC)),
            dma((nb, NC)),
            dma((2,)),
        ],
        compiler_params=pltpu.CompilerParams(
            collective_id=0, has_side_effects=True, vmem_limit_bytes=60 * 1024 * 1024
        ),
    )(
        image_feats,
        key_weight,
        value_weight,
        key_gain.reshape(1, HD),
        slot_image.reshape(TC, HD),
        queries,
        text_image.reshape(1, text_image.shape[0]),
        text_hidden,
        out_weight,
        attn_gate,
    )


def solution(mesh):
    placed = (
        P(("groups", "blk"), None),
        P(("groups", "blk")),
        P("blk", "heads"),
        P("blk", "heads"),
        P(),
        P(("groups", "blk"), "heads"),
        P("groups"),
        P(("groups", "heads"), "blk"),
        P("heads", "blk"),
        P(),
    )
    return jax.shard_map(
        functools.partial(body, mesh.shape["blk"]),
        mesh=mesh,
        in_specs=placed,
        out_specs=P(("groups", "heads"), "blk"),
        check_vma=False,
    )
```

```python
import functools
import math

import jax
import jax.numpy as jnp
from jax import lax
from jax.experimental import pallas as pl
from jax.experimental.pallas import tpu as pltpu
from jax.sharding import PartitionSpec as P

HD = 128
F32 = jnp.float32
BF16 = jnp.bfloat16
MESH = pl.DeviceIdType.MESH


def kernel(
    nb,
    chunks,
    feats,
    kw,
    vw,
    gain,
    slots,
    queries,
    text,
    hidden,
    wout,
    gate,
    out,
    wbuf,
    fown,
    fnbr,
    acc_own,
    acc_nbr,
    psend,
    precv,
    pbuf,
    gbuf,
    qbuf,
    qall,
    sbuf,
    mbuf,
    img,
    agbuf,
    wov,
    part,
    xsend,
    xrecv,
    lsem,
    fsem,
    wz_send,
    wx_send,
    w_recv,
    f_send,
    ff_send,
    f_recv,
    q_sem,
    p_send,
    p_recv,
    k_send,
    kf_send,
    k_recv,
    az_send,
    af_send,
    a_recv,
    x_sem,
    hid,
    h_sem,
):
    Y = 2
    Z = nb // Y
    ZH = Z // 2
    half = nb // 2
    g = lax.axis_index("groups")
    b = lax.axis_index("blk")
    c = lax.axis_index("heads")
    z = b // Y
    y = b % Y
    h = z // ZH
    r = (z % ZH) * Y + y
    gp = g % 2
    gx = g + 1 - 2 * gp
    tok, dv = feats.shape
    S, kc = kw.shape
    rows, qc = queries.shape
    gc = qc // 2
    qpk = gc // HD
    R2 = 2 * rows
    CR = S // chunks
    ybro = {"blk": z * Y + 1 - y}
    xbro = {"groups": gx}
    cbro = {"heads": 1 - c}
    qbro = (1 - h) * half + r
    pending = []

    def remote(src, dst, ssem, rsem, dev):
        return pltpu.make_async_remote_copy(
            src_ref=src, dst_ref=dst, send_sem=ssem, recv_sem=rsem, device_id=dev, device_id_type=MESH
        )

    def send(cond, *args):
        copy = remote(*args)
        if cond is None:
            copy.start()
        else:
            pl.when(cond)(lambda: copy.start())
        pending.append((cond, copy))

    def arrived(ref, sem):
        pltpu.make_async_copy(ref, ref, sem).wait()

    own_k = pltpu.make_async_copy(kw, wbuf.at[0, z], lsem.at[0])
    own_v = pltpu.make_async_copy(vw, wbuf.at[1, z], lsem.at[1])
    own_k.start()
    own_v.start()

    barrier = pltpu.get_barrier_semaphore()
    for zd in range(Z):

        @pl.when(zd != z)
        def _():
            pl.semaphore_signal(barrier, inc=1, device_id={"blk": zd * Y + y}, device_id_type=MESH)

    for dev in (ybro, xbro, cbro):
        pl.semaphore_signal(barrier, inc=1, device_id=dev, device_id_type=MESH)
    own_k.wait()
    own_v.wait()
    pl.semaphore_wait(barrier, Z + 2)

    def wslot(kv, zi, ci):
        return wbuf.at[kv, zi, pl.ds(ci * CR, CR), :]

    for ci in range(chunks):
        for dirn, ok in ((1, z + 1 < Z), (-1, z >= 1)):
            slot = wslot(gp, z, ci)
            send(
                ok,
                slot,
                slot,
                wz_send.at[z, ci, (1 - dirn) // 2],
                w_recv.at[gp, z, ci],
                {"blk": b + dirn * Y},
            )

    FB = Z // 2
    for i in range(FB):
        zi = 2 * i + c
        send(
            None,
            feats.at[:, pl.ds(pl.multiple_of((zi * Y + 1 - y) * S, S), S)],
            fnbr.at[zi],
            f_send.at[i],
            f_recv.at[zi],
            ybro,
        )
    send(
        None,
        queries.at[:, pl.ds(pl.multiple_of((1 - h) * gc, gc), gc)],
        qbuf.at[h],
        q_sem.at[0],
        q_sem.at[1],
        {"blk": qbro},
    )
    floc = []
    for zi in range(Z):
        cp = pltpu.make_async_copy(
            feats.at[:, pl.ds(pl.multiple_of((zi * Y + y) * S, S), S)], fown.at[zi], fsem.at[zi]
        )
        cp.start()
        floc.append(cp)
    qloc = pltpu.make_async_copy(
        queries.at[:, pl.ds(pl.multiple_of(h * gc, gc), gc)], qbuf.at[h], lsem.at[2]
    )
    qloc.start()
    woloc = pltpu.make_async_copy(wout, wov, lsem.at[3])
    woloc.start()
    hloc = pltpu.make_async_copy(hidden, hid, h_sem)
    hloc.start()

    acc_own[...] = jnp.zeros_like(acc_own)
    acc_nbr[...] = jnp.zeros_like(acc_nbr)

    def mm(acc, feat, zi):
        for kv in range(2):
            acc[:, kv * kc : (kv + 1) * kc] += jnp.dot(
                feat[zi], wbuf[kv, zi], preferred_element_type=F32
            )

    for cp in floc:
        cp.wait()

    def sides(s):
        return ((z - s, z - s >= 0, -1), (z + s, z + s < Z, 1))

    for s in range(1, Z):
        for ci in range(chunks):
            for zi, ok, side in sides(s):
                slot = wslot(gp, zi, ci)
                pl.when(ok)(lambda: arrived(slot, w_recv.at[gp, zi, ci]))
                onward = b - side * Y
                more = ok & ((z + 1 < Z) if side < 0 else (z >= 1))
                send(more, slot, slot, wz_send.at[zi, ci, 0], w_recv.at[gp, zi, ci], {"blk": onward})
                send(ok, slot, slot, wx_send.at[zi, ci], w_recv.at[gp, zi, ci], xbro)
        if s - 1 < FB:
            zi = 2 * (s - 1) + c
            arrived(fnbr.at[zi], f_recv.at[zi])
            send(None, fnbr.at[zi], fnbr.at[zi], ff_send.at[s - 1], f_recv.at[zi], cbro)
        if s == 1:
            mm(acc_own, fown, z)
        else:
            for zi, ok, _ in sides(s - 1):

                @pl.when(ok)
                def _():
                    for ci in range(chunks):
                        arrived(wslot(1 - gp, zi, ci), w_recv.at[1 - gp, zi, ci])
                    mm(acc_own, fown, zi)

    for i in range(FB):
        zi = 2 * i + 1 - c
        arrived(fnbr.at[zi], f_recv.at[zi])
    for zi, ok, _ in sides(Z - 1):

        @pl.when(ok)
        def _():
            for ci in range(chunks):
                arrived(wslot(1 - gp, zi, ci), w_recv.at[1 - gp, zi, ci])

    TC = tok // HD
    for t in range(TC):
        lo, hi = t * HD, (t + 1) * HD

        @pl.loop(0, Z)
        def _(zi):
            for kv in range(2):
                acc_nbr[lo:hi, kv * kc : (kv + 1) * kc] += jnp.dot(
                    fnbr[zi, lo:hi, :], wbuf[kv, zi], preferred_element_type=F32
                )

        psend[t] = acc_nbr[lo:hi, :].astype(BF16)
        send(None, psend.at[t], precv.at[t], p_send.at[t], p_recv.at[t], ybro)
    for zi, ok, _ in sides(Z - 1):
        pl.when(ok)(lambda: mm(acc_own, fown, zi))

    for t in range(TC):
        arrived(precv.at[t], p_recv.at[t])
        total = acc_own[t * HD : (t + 1) * HD, :] + precv[t].astype(F32)
        code = jnp.broadcast_to(slots[t : t + 1, :].astype(F32), (16, HD)).astype(BF16)
        for hh in range(2):
            kr = total[:, hh * HD : (hh + 1) * HD]
            scale = lax.rsqrt(jnp.mean(kr * kr, axis=-1, keepdims=True) + 1e-05)
            pbuf[hh, t, 0:HD, :] = (kr * scale * gain[...]).astype(BF16)
            pbuf[hh, t, HD : 2 * HD, :] = total[:, kc + hh * HD : kc + (hh + 1) * HD].astype(BF16)
            pbuf[hh, t, 2 * HD :, :] = code
        gbuf[b, t] = pbuf[h, t]
        for zd in range(Z):
            send(
                zd != z,
                pbuf.at[zd // ZH, t],
                gbuf.at[b, t],
                k_send.at[zd, t],
                k_recv.at[b, t],
                {"blk": zd * Y + y},
            )
        send(None, gbuf.at[b, t], gbuf.at[b, t], kf_send.at[z, t], k_recv.at[b, t], ybro)

    qloc.wait()
    arrived(qbuf.at[1 - h], q_sem.at[1])
    for j in range(qpk):
        for so in range(2):
            at = j * R2 + so * rows
            qall[at : at + rows, :] = qbuf[so, :, j * HD : (j + 1) * HD]
    count = text.shape[1]
    lane = lax.broadcasted_iota(jnp.int32, (R2, count), 1)
    sub = lax.broadcasted_iota(jnp.int32, (R2, count), 0)
    want = jnp.where(sub < rows, sub, sub + (half - 1) * rows) + r * rows
    picked = jnp.where(lane == want, text[...].astype(F32), 0.0)
    rowcol = jnp.broadcast_to(jnp.sum(picked, axis=1, keepdims=True), (R2, HD))
    for j in range(qpk):
        img[j * R2 : (j + 1) * R2, :] = rowcol
    mbuf[...] = jnp.full_like(mbuf, -1e30)
    score_scale = 1.0 / math.sqrt(HD)

    def score(bi):
        top = mbuf[...]
        for t in range(TC):
            s = (
                lax.dot_general(
                    qall[...],
                    gbuf[bi, t, 0:HD, :],
                    (((1,), (1,)), ((), ())),
                    preferred_element_type=F32,
                )
                * score_scale
            )
            crow = gbuf[bi, t, 2 * HD :, :].astype(F32)[0:1, :]
            s = jnp.where((crow >= 0.0) & (crow <= img[...]), s, -1e30)
            sbuf[bi, t] = s
            top = jnp.maximum(top, s)
        mbuf[...] = top

    for s in range(1, Z):
        for t in range(TC):
            for zi, ok, _ in sides(s):
                slot = gbuf.at[zi * Y + y, t]
                sem = k_recv.at[zi * Y + y, t]
                pl.when(ok)(lambda: arrived(slot, sem))
                send(ok, slot, slot, kf_send.at[zi, t], sem, ybro)

    @pl.loop(0, Z)
    def _(zi):
        score(zi * Y + y)

    @pl.loop(0, Z)
    def _(zi):
        for t in range(TC):
            arrived(gbuf.at[zi * Y + 1 - y, t], k_recv.at[zi * Y + 1 - y, t])
        score(zi * Y + 1 - y)

    NC = agbuf.shape[1]
    HC = qpk // NC
    MC = HC * R2

    def aslot(bi, jc):
        zz = bi // Y
        return agbuf.at[zz // ZH, jc, :, (zz % ZH) * Y + bi % Y]

    for jc in range(NC):
        r0, r1 = jc * MC, (jc + 1) * MC
        top = jnp.max(mbuf[r0:r1, :], axis=1, keepdims=True)

        def step(bi, carry):
            tot, acc = carry
            ps = [jnp.exp(sbuf[bi, t, r0:r1, :] - top) for t in range(TC)]
            for p in ps:
                tot = tot + p
            acc = acc + jnp.dot(
                jnp.concatenate([p.astype(BF16) for p in ps], axis=1),
                jnp.concatenate([gbuf[bi, t, HD : 2 * HD, :] for t in range(TC)], axis=0),
                preferred_element_type=F32,
            )
            return tot, acc

        zero = jnp.zeros((MC, HD), F32)
        tot, acc = lax.fori_loop(0, nb, step, (zero, zero))
        attn = (acc / jnp.sum(tot, axis=1, keepdims=True)).astype(BF16)
        for jj in range(HC):
            for so in range(2):
                at = jj * R2 + so * rows
                agbuf[h, jc, so, r, :, jj * HD : (jj + 1) * HD] = attn[at : at + rows, :]
        slot = aslot(b, jc)
        sem = a_recv.at[b, jc]
        send(z + 1 < Z, slot, slot, az_send.at[z, jc, 0], sem, {"blk": b + Y})
        send(z >= 1, slot, slot, az_send.at[z, jc, 1], sem, {"blk": b - Y})
        send(None, slot, slot, af_send.at[z, jc], sem, ybro)

    for s in range(1, Z):
        for jc in range(NC):
            for zi, ok, side in sides(s):
                bi = zi * Y + y
                slot = aslot(bi, jc)
                sem = a_recv.at[bi, jc]
                pl.when(ok)(lambda: arrived(slot, sem))
                more = ok & ((z + 1 < Z) if side < 0 else (z >= 1))
                send(more, slot, slot, az_send.at[zi, jc, 0], sem, {"blk": b - side * Y})
                send(ok, slot, slot, af_send.at[zi, jc], sem, ybro)
    for zi in range(Z):
        for jc in range(NC):
            bi = zi * Y + 1 - y
            arrived(aslot(bi, jc), a_recv.at[bi, jc])

    woloc.wait()
    hloc.wait()
    hrows = half * rows
    ocols = out.shape[1]

    def proj(so):
        a = [agbuf[hh, jc, so].reshape(hrows, HC * HD) for hh in range(2) for jc in range(NC)]
        return jnp.dot(jnp.concatenate(a, axis=1), wov[...], preferred_element_type=F32)

    xsend[...] = proj(1 - c).astype(BF16)
    send(None, xsend, xrecv, x_sem.at[0], x_sem.at[1], cbro)
    part[...] = proj(c)
    arrived(xrecv, x_sem.at[1])
    out[...] = (
        hid[...].astype(F32) + jnp.tanh(jnp.full((1, ocols), gate[0], F32)) * (part[...] + xrecv[...].astype(F32))
    ).astype(BF16)

    for cond, copy in pending:
        if cond is None:
            copy.wait_send()
        else:
            pl.when(cond)(lambda: copy.wait_send())


def body(
    nb,
    image_feats,
    slot_image,
    key_weight,
    value_weight,
    key_gain,
    queries,
    text_image,
    text_hidden,
    out_weight,
    attn_gate,
):
    Z = nb // 2
    ZH = Z // 2
    half = nb // 2
    tok, dv = image_feats.shape
    S, kc = key_weight.shape
    rows, qc = queries.shape
    gc = qc // 2
    qpk = gc // HD
    M = qpk * 2 * rows
    trows, ocols = text_hidden.shape
    chunks = 8 if S % 128 == 0 else 4
    TC = tok // HD
    NC = max(1, qpk // 2)
    any_spec = pl.BlockSpec(memory_space=pl.ANY)
    vspec = pl.BlockSpec(memory_space=pltpu.VMEM)
    dma = pltpu.SemaphoreType.DMA
    V = pltpu.VMEM
    return pl.pallas_call(
        functools.partial(kernel, nb, chunks),
        out_shape=jax.ShapeDtypeStruct((trows, ocols), BF16),
        in_specs=[
            any_spec,
            any_spec,
            any_spec,
            vspec,
            vspec,
            any_spec,
            vspec,
            any_spec,
            any_spec,
            pl.BlockSpec(memory_space=pltpu.SMEM),
        ],
        out_specs=vspec,
        scratch_shapes=[
            V((2, Z, S, kc), BF16),
            V((Z, tok, S), BF16),
            V((Z, tok, S), BF16),
            V((tok, 2 * kc), F32),
            V((tok, 2 * kc), F32),
            V((TC, HD, 2 * kc), BF16),
            V((TC, HD, 2 * kc), BF16),
            V((2, TC, 2 * HD + 16, HD), BF16),
            V((nb, TC, 2 * HD + 16, HD), BF16),
            V((2, rows, gc), BF16),
            V((M, HD), BF16),
            V((nb, tok // HD, M, HD), F32),
            V((M, HD), F32),
            V((M, HD), F32),
            V((2, NC, 2, half, rows, gc // NC), BF16),
            V(out_weight.shape, BF16),
            V((trows, ocols), F32),
            V((trows, ocols), BF16),
            V((trows, ocols), BF16),
            dma((4,)),
            dma((Z,)),
            dma((Z, chunks, 2)),
            dma((Z, chunks)),
            dma((2, Z, chunks)),
            dma((Z // 2,)),
            dma((Z // 2,)),
            dma((Z,)),
            dma((2,)),
            dma((TC,)),
            dma((TC,)),
            dma((Z, TC)),
            dma((Z, TC)),
            dma((nb, TC)),
            dma((Z, NC, 2)),
            dma((Z, NC)),
            dma((nb, NC)),
            dma((2,)),
            V((trows, ocols), BF16),
            dma,
        ],
        compiler_params=pltpu.CompilerParams(
            collective_id=0, has_side_effects=True, vmem_limit_bytes=60 * 1024 * 1024
        ),
    )(
        image_feats,
        key_weight,
        value_weight,
        key_gain.reshape(1, HD),
        slot_image.reshape(TC, HD),
        queries,
        text_image.reshape(1, text_image.shape[0]),
        text_hidden,
        out_weight,
        attn_gate,
    )


def solution(mesh):
    placed = (
        P(("groups", "blk"), None),
        P(("groups", "blk")),
        P("blk", "heads"),
        P("blk", "heads"),
        P(),
        P(("groups", "blk"), "heads"),
        P("groups"),
        P(("groups", "heads"), "blk"),
        P("heads", "blk"),
        P(),
    )
    return jax.shard_map(
        functools.partial(body, mesh.shape["blk"]),
        mesh=mesh,
        in_specs=placed,
        out_specs=P(("groups", "heads"), "blk"),
        check_vma=False,
    )
```
